32 devices in a mesh: groups: 2 (over x), seq: 8 (over z, y), head: 2 (over core).
Axes of the slice: x: 2, y: 2, z: 4, core: 2. Of those that a mesh axis runs over, the one named last changes fastest.
Arguments:
- queries: bfloat16 [4096, 3584], P(('groups', 'seq'), 'head'), parts along dimension 0, may hold values from -30 to 30
- current_keys: bfloat16 [4096, 512], P(('groups', 'seq'), 'head'), parts along dimension 0, may hold values from -6 to 6
- current_values: bfloat16 [4096, 512], P(('groups', 'seq'), 'head'), parts along dimension 0, may hold values from -6 to 6
- stored_keys: bfloat16 [4096, 2, 512], P(('groups', 'seq'), None, 'head'), parts along dimension 0, may hold values from -22 to 22
- stored_values: bfloat16 [4096, 2, 512], P(('groups', 'seq'), None, 'head'), parts along dimension 0, may hold values from -6 to 6
- remap_table: int32 [3, 64], P(None, ('groups', 'seq')), parts along dimension 1, may hold values from 0 to 2047
- block_table: int32 [256], P('groups'), parts along dimension 0, may hold values from 0 to 15, as said below
Outputs:
- attended: bfloat16 [4096, 3584], P(('groups', 'seq'), 'head'), parts along dimension 0
- paged_keys: bfloat16 [4, 256, 2048], P('head', ('groups', 'seq')), parts along dimension 1
- paged_values: bfloat16 [4, 256, 2048], P('head', ('groups', 'seq')), parts along dimension 1
The draws below stay inside these ranges and needn't reach their ends.
There are 2 independent parts, one for each index of `groups`. The reference program is written for one: setup_inputs(seed, part) draws one part's arguments, and reference() takes and returns one part's arrays. A program takes and returns all parts, laid end to end along the dimension named above; each array names one. Nothing has to cross between parts.
Inputs may be any that keep to these rules, and one draw needn't show every extreme that they name: `block_table`: the entries of the blocks b that share b modulo 8 are a permutation of 0 to 15.
All inputs are finite; a program needn't handle non-finite values.
Results may differ from the reference program's by a relative error of at most 0.012.
The reference program's roundings to bfloat16 on the way count: a program that leaves them out, or rounds other values in their place, can miss the bound.
Values may be sent and summed in bfloat16 or wider, within the bound.
A program may use at most 128 MiB of HBM per device.

```python
import jax
import jax.numpy as jnp
from jax import lax

HQ = 28
KEY_VALUE_HEADS = 4
HEAD_SIZE = 128
PRIOR_SEGMENTS = 2
PAGE_TOKENS = 16
QBLK = 64
QUERY_PER_KEY = 7
SEGMENT_TOKENS = 2048
NQB = 32
SEGMENT_PAGES = 128
OWNERS = 8
PAGES_DEV = 16


def draw_queries(key, part):
    rotary_base = jnp.clip(jax.random.normal(jax.random.fold_in(key, 1), (SEGMENT_TOKENS, HQ * HEAD_SIZE), jnp.float32), -6.0, 6.0) * 2.2
    return rotary_base.astype(jnp.bfloat16)


def draw_stored_keys(key, part):
    rotary_base = jnp.clip(jax.random.normal(jax.random.fold_in(key, 2), (SEGMENT_TOKENS, PRIOR_SEGMENTS, KEY_VALUE_HEADS * HEAD_SIZE), jnp.float32), -6.0, 6.0)
    return rotary_base.astype(jnp.bfloat16)


def draw_block_table(key, part):
    holder_keys = jax.random.split(jax.random.fold_in(key, 5), OWNERS)
    orders = jax.vmap(lambda single: jax.random.permutation(single, PAGES_DEV))(holder_keys)
    return orders.T.reshape(-1).astype(jnp.int32)


def touch_ends(entries, own_key, smallest, top_value):
    spot = [jax.random.randint(jax.random.fold_in(own_key, axis), (), 0, length) for axis, length in enumerate(entries.shape)]
    main_axis = entries.shape.index(max(entries.shape))
    beside = spot[:main_axis] + [(spot[main_axis] + 1) % entries.shape[main_axis]] + spot[main_axis + 1:]
    return entries.at[tuple(spot)].set(smallest).at[tuple(beside)].set(top_value)


def block_levels(own_key, dims, cuts, least, top_value):
    def one(dim, shards_of):
        steps = jax.random.uniform(jax.random.fold_in(jax.random.fold_in(own_key, 6), dim), (shards_of,), jnp.float32, least / len(cuts), top_value / len(cuts))
        return jnp.repeat(jnp.exp(steps), dims[dim] // shards_of).reshape((-1,) + (1,) * (len(dims) - dim - 1))

    gain = one(*cuts[0])
    for cut in cuts[1:]:
        gain = gain * one(*cut)
    return gain


def scatter_about(stream_key, extent, spread, most, cuts=(), kind=jnp.bfloat16):
    loudness = block_levels(stream_key, extent, cuts, -0.22, 0.18) if cuts else 1.0
    values = jax.random.normal(stream_key, extent, jnp.float32) * spread * loudness
    return jnp.minimum(jnp.maximum(values, -most), most).astype(kind)


def setup_inputs(seed: int = 0, part: int = 0) -> dict:
    key_list = jax.random.split(jax.random.key(seed), 8)
    part_splits = jax.random.split(jax.random.fold_in(key_list[7], part), 8)
    queries = draw_queries(jax.random.fold_in(jax.random.fold_in(key_list[7], part), 71), part)
    current_keys = scatter_about(part_splits[1], (SEGMENT_TOKENS, KEY_VALUE_HEADS * HEAD_SIZE), 1.0, 6.0, ((0, 8), (1, 2)))
    current_values = scatter_about(part_splits[2], (SEGMENT_TOKENS, KEY_VALUE_HEADS * HEAD_SIZE), 1.0, 6.0, ((0, 8), (1, 2)))
    stored_keys = draw_stored_keys(jax.random.fold_in(jax.random.fold_in(key_list[7], part), 71), part)
    stored_values = scatter_about(part_splits[4], (SEGMENT_TOKENS, PRIOR_SEGMENTS, KEY_VALUE_HEADS * HEAD_SIZE), 1.0, 6.0, ((0, 8), (2, 2)))
    remap_table = touch_ends(jax.random.randint(part_splits[5], (3, NQB), 0, SEGMENT_TOKENS), jax.random.fold_in(part_splits[5], 1), 0, SEGMENT_TOKENS - 1).astype(jnp.int32)
    block_table = draw_block_table(jax.random.fold_in(jax.random.fold_in(key_list[7], part), 71), part)
    return dict(queries=queries, current_keys=current_keys, current_values=current_values, stored_keys=stored_keys, stored_values=stored_values, remap_table=remap_table, block_table=block_table)


rope_base = 1000000.0
masked_value = -1e30


def apply_rotary(values, token_positions):
    half_dim = values.shape[-1] // 2
    frequency = rope_base ** (-2.0 * jnp.arange(half_dim, dtype=jnp.float32) / values.shape[-1])
    angles = token_positions.astype(jnp.float32)[:, None] * frequency[None, :]
    cos_table = jnp.cos(angles)[:, None, :]
    sin_table = jnp.sin(angles)[:, None, :]
    first_half = values[..., :half_dim]
    second_half = values[..., half_dim:]
    return jnp.concatenate([first_half * cos_table - second_half * sin_table, second_half * cos_table + first_half * sin_table], -1)


def paged_layout(cache_portion, block_table):
    page_blocks = cache_portion.reshape(SEGMENT_PAGES, PAGE_TOKENS, KEY_VALUE_HEADS, HEAD_SIZE).transpose(2, 0, 1, 3).reshape(KEY_VALUE_HEADS, SEGMENT_PAGES, PAGE_TOKENS * HEAD_SIZE)
    block_index = jnp.arange(SEGMENT_PAGES, dtype=jnp.int32)
    target = (block_index % OWNERS) * PAGES_DEV + block_table
    return jnp.zeros_like(page_blocks).at[:, target].set(page_blocks)


def reference(queries, current_keys, current_values, stored_keys, stored_values, remap_table, block_table):
    token_index = jnp.arange(SEGMENT_TOKENS, dtype=jnp.int32)
    token_positions = jnp.repeat(remap_table, QBLK, axis=1) + (token_index % QBLK)[None, :]
    query_single_float = queries.astype(jnp.float32).reshape(SEGMENT_TOKENS, HQ, HEAD_SIZE)
    rotary_output = [apply_rotary(query_single_float, token_positions[segment_kind_index]).astype(jnp.bfloat16).reshape(SEGMENT_TOKENS, KEY_VALUE_HEADS, QUERY_PER_KEY, HEAD_SIZE) for segment_kind_index in range(3)]
    score_scale = HEAD_SIZE ** -0.5
    value_portions = [stored_values[:, segment_number, :] for segment_number in range(PRIOR_SEGMENTS)] + [current_values]
    joined_values = jnp.concatenate(value_portions, 0).reshape((PRIOR_SEGMENTS + 1) * SEGMENT_TOKENS, KEY_VALUE_HEADS, HEAD_SIZE).astype(jnp.float32)
    query_block = min(256, SEGMENT_TOKENS)

    def one_block(block_number):
        first_row = block_number * query_block
        score_parts = []
        for segment_number in range(PRIOR_SEGMENTS):
            chosen = rotary_output[2] if segment_number < PRIOR_SEGMENTS - 1 else rotary_output[1]
            query_rows = lax.dynamic_slice_in_dim(chosen, first_row, query_block, 0).astype(jnp.float32)
            key_row_list = stored_keys[:, segment_number, :].reshape(SEGMENT_TOKENS, KEY_VALUE_HEADS, HEAD_SIZE).astype(jnp.float32)
            score_parts.append(jnp.einsum("qgrd,kgd->grqk", query_rows, key_row_list) * score_scale)
        query_rows = lax.dynamic_slice_in_dim(rotary_output[0], first_row, query_block, 0).astype(jnp.float32)
        key_row_list = current_keys.reshape(SEGMENT_TOKENS, KEY_VALUE_HEADS, HEAD_SIZE).astype(jnp.float32)
        intra = jnp.einsum("qgrd,kgd->grqk", query_rows, key_row_list) * score_scale
        allowed = token_index[None, :] <= (first_row + jnp.arange(query_block, dtype=jnp.int32))[:, None]
        score_parts.append(jnp.where(allowed[None, None], intra, masked_value))
        scores = jnp.concatenate(score_parts, -1)
        weights = jnp.exp(scores - jnp.max(scores, -1, keepdims=True))
        denom = jnp.sum(weights, -1)
        rounded = weights.astype(jnp.bfloat16).astype(jnp.float32)
        summed = jnp.einsum("grqk,kgd->qgrd", rounded, joined_values)
        result = summed / denom.transpose(2, 0, 1)[..., None]
        return result.astype(jnp.bfloat16).reshape(query_block, HQ * HEAD_SIZE)

    attended = lax.map(one_block, jnp.arange(SEGMENT_TOKENS // query_block, dtype=jnp.int32)).reshape(SEGMENT_TOKENS, HQ * HEAD_SIZE)
    paged_keys = paged_layout(stored_keys[:, PRIOR_SEGMENTS - 1, :], block_table)
    paged_values = paged_layout(stored_values[:, PRIOR_SEGMENTS - 1, :], block_table)
    return (attended, paged_keys, paged_values)
```

```python
import functools
import heapq
import math

import jax
import jax.numpy as jnp
from jax import lax
from jax.experimental import pallas as pl
from jax.experimental.pallas import tpu as pltpu
from jax.sharding import PartitionSpec as P

HEAD_SIZE = 128
PRIOR_SEGMENTS = 2
PAGE_TOKENS = 16
QBLK = 64
KINDS = PRIOR_SEGMENTS + 1
CURRENT = PRIOR_SEGMENTS

rope_base = 1000000.0
masked_value = -1e30
MESH = pl.DeviceIdType.MESH
RIGHT, LEFT, ACROSS = 0, 1, 2
ONES_ROWS = 16

OWN0, OWN1, GUEST, SPARE = 0, 1, 2, 3
NOTHING, BATCH2, BATCH1, TURN, DIAGONAL, GUEST_TURN, PACK, RETURN, PAGES, MERGE = range(10)
FIELD = 128

WIRE, HOP, RELAY = 2.81, 1.9, 1.0
COST = {BATCH2: 2.6, BATCH1: 1.5, TURN: 4.0, DIAGONAL: 1.6, GUEST_TURN: 2.0, PACK: 0.8, PAGES: 1.3}


def offloaded(n, d):
    if d < n - 2 or n < 4:
        return set()
    return {
        (j, part, 0)
        for j in range(n - 2)
        for part in (0, CURRENT)
        if part < CURRENT or j <= n - 4
    }


def needed(n, groups, d):
    left = offloaded(n, d)
    return {
        (j, part, g)
        for j in range(n)
        for part in range(KINDS)
        for g in range(groups)
        if j != d and (part < CURRENT or j < d) and (j, part, g) not in left
    }


def route(n, groups):
    need = {d: needed(n, groups, d) for d in range(n)}
    here = {
        d: {(d, part, g): 0.0 for part in range(KINDS) for g in range(groups)} for d in range(n)
    }
    taken = {d: set(here[d]) for d in range(n)}
    lack = {}
    for d in range(n):
        for x in sorted(need[d]):
            lack[x] = lack.get(x, 0) + 1
    target = {}
    for d in range(n):
        if d + 2 < n:
            target[(d, RIGHT)] = d + 2
        if d - 2 >= 0:
            target[(d, LEFT)] = d - 2
        target[(d, ACROSS)] = d ^ 1
    wanted = {d - 2: offloaded(n, d) for d in range(n) if offloaded(n, d)}
    urgent = set().union(*wanted.values()) if wanted else set()
    free = {link: 0.0 for link in target}
    for h in wanted:
        free[(h + 2, LEFT)] = 3.5 * WIRE
    ready = {}
    returned = {}
    sends = {link: [] for link in target}
    arrivals = {d: {} for d in range(n)}
    events = []
    for k, link in enumerate(target):
        heapq.heappush(events, (free[link], k, 0, link))
    count = len(events)
    idle = set()

    def pick(link, now):
        u, v = link[0], target[link]
        if link[1] == RIGHT and u in wanted and u not in returned and ready.get(u, now + 1) <= now:
            return RETURN
        best = None
        for x in sorted(here[u]):
            if here[u][x] > now + 1e-9 or x in taken[v] or x not in need[v]:
                continue
            others = sum(1 for w in (v + 2, v - 2, v ^ 1) if 0 <= w < n and w != u and x in taken[w])
            score = lack[x] - SHARED * others
            if x in urgent and (v in wanted or (link[1] != LEFT and v < n - 4)):
                score += BONUS
            score += ((x[0] * 7 + x[1] * 5 + x[2] * 3 + u * 11 + link[1] * 13 + SALT) * 7919 % 101) / 101
            if best is None or score > best[0]:
                best = (score, x)
        return None if best is None else best[1]

    while events:
        now, _, kind, what = heapq.heappop(events)
        if kind == 0:
            link = what
            if free[link] > now + 1e-9:
                heapq.heappush(events, (free[link], count, 0, link))
                count += 1
                continue
            x = pick(link, now)
            if x is None:
                idle.add(link)
                continue
            v = target[link]
            if x == RETURN:
                returned[link[0]] = now + 3.6 * WIRE + HOP
                free[link] = now + 3.6 * WIRE
            else:
                taken[v].add(x)
                lack[x] -= 1
                sends[link].append(x)
                arrivals[v][x] = now + WIRE + HOP
                here[v][x] = now + WIRE + HOP + RELAY
                free[link] = now + WIRE
                heapq.heappush(events, (here[v][x], count, 1, v))
                count += 1
                if v in wanted and v not in ready and wanted[v] <= set(here[v]):
                    ready[v] = max(here[v][y] for y in wanted[v]) + 4.0
                    heapq.heappush(events, (ready[v], count, 1, v))
                    count += 1
            heapq.heappush(events, (free[link], count, 0, link))
            count += 1
        else:
            for link in sorted(x for x in idle if x[0] == what):
                idle.discard(link)
                heapq.heappush(events, (max(now, free[link]), count, 0, link))
                count += 1
    return sends, arrivals, wanted, returned


SALT, BONUS, SHARED = 16, 3.0, 2.0


def schedule(n, groups):
    sends, arrivals, wanted, returned = route(n, groups)
    tables = []
    for d in range(n):
        rows = []
        have = {(d, part, g) for part in range(KINDS) for g in range(groups)}
        queue = {way: list(sends.get((d, way), [])) for way in (RIGHT, LEFT, ACROSS)}
        order = sorted(arrivals[d], key=lambda x: (arrivals[d][x], x))
        guest = sorted(wanted.get(d, ()))
        pending = {OWN0: [], OWN1: [], GUEST: []}
        absorbed_guest = 0
        turned_guest = packed = sent_back = paged = False
        pages_left = {(j, 1, g) for j in range(n) for g in range(groups)} - have

        def ready_sends():
            out = {}
            for way, q in queue.items():
                if q and q[0] in have:
                    out[way] = q.pop(0)
            return out

        def emit(wait=None, op=NOTHING, pieces=(), accs=()):
            if wait is not None:
                have.add(wait)
            rows.append([wait, ready_sends(), op, list(pieces), list(accs)])
            while True:
                more = ready_sends()
                if not more:
                    break
                rows.append([None, more, NOTHING, [], []])

        def note(x):
            pages_left.discard(x)
            pending[x[2]].append(x)
            if x in guest:
                pending[GUEST].append(x)

        def streams(count, size):
            chosen = []
            for acc in (GUEST, OWN0, OWN1):
                if acc == GUEST and not turned_guest:
                    continue
                while len(pending[acc]) >= size and len(chosen) < count:
                    chosen.append((acc, [pending[acc].pop(0) for _ in range(size)]))
            return chosen

        def put_back(chosen):
            for acc, pieces in reversed(chosen):
                pending[acc] = pieces + pending[acc]

        def batch(op, chosen):
            nonlocal now, absorbed_guest
            pieces, accs = [], []
            for acc, some in chosen:
                pieces += some
                accs.append(acc)
                absorbed_guest += len(some) if acc == GUEST else 0
            emit(None, op, pieces, accs)
            now += COST[op]

        emit()
        emit(None, TURN)
        now = COST[TURN]
        for g in range(groups):
            for part in range(PRIOR_SEGMENTS):
                note((d, part, g))
            if (d, CURRENT, g) in guest:
                pending[GUEST].append((d, CURRENT, g))
        first = [(OWN0, [pending[OWN0].pop(0) for _ in range(2)]),
                 (OWN1, [pending[OWN1].pop(0) for _ in range(2)])]
        batch(BATCH2, first)
        emit(None, DIAGONAL)
        now += COST[DIAGONAL]
        guest_at = 3.5 * WIRE + HOP + 1.0
        while True:
            while order and arrivals[d][order[0]] <= now + 0.2:
                x = order.pop(0)
                emit(x)
                note(x)
            if guest and not turned_guest and guest_at <= now:
                emit(None, GUEST_TURN)
                now += COST[GUEST_TURN]
                turned_guest = True
                continue
            if packed and not sent_back:
                emit(None, RETURN)
                sent_back = True
                continue
            if guest and not packed and absorbed_guest == len(guest):
                emit(None, PACK)
                now += COST[PACK]
                packed = True
                continue
            chosen = streams(2, 2)
            if len(chosen) == 2:
                batch(BATCH2, chosen)
                continue
            put_back(chosen)
            last_guest = (
                guest and turned_guest and absorbed_guest + len(pending[GUEST]) == len(guest)
            )
            upcoming = arrivals[d][order[0]] if order else None
            if last_guest and pending[GUEST]:
                chosen = streams(2, 1)
                if len(chosen) == 1:
                    chosen.append((SPARE, list(chosen[0][1])))
                batch(BATCH1, chosen)
                continue
            if not pages_left and not paged:
                emit(None, PAGES)
                now += COST[PAGES]
                paged = True
                continue
            if guest and not turned_guest and (upcoming is None or guest_at <= upcoming):
                now = max(now, guest_at)
                continue
            if upcoming is None or upcoming - now > 1.2:
                chosen = streams(2, 1)
                if len(chosen) == 2:
                    batch(BATCH1, chosen)
                    continue
                if chosen and upcoming is None:
                    chosen.append((SPARE, list(chosen[0][1])))
                    batch(BATCH1, chosen)
                    continue
                put_back(chosen)
            if upcoming is None:
                break
            now = max(now, upcoming)
        if offloaded(n, d):
            emit(None, MERGE)
        assert not any(queue.values()) and not any(pending.values()) and paged
        tables.append(rows)
    length = max(len(rows) for rows in tables)

    def number(x):
        return (x[0] * KINDS + x[1]) * groups + x[2]

    packed_tables = []
    for rows in tables:
        words = []
        for wait, sent, op, pieces, accs in rows:
            first = 0 if wait is None else number(wait) + 1
            for way in (RIGHT, LEFT, ACROSS):
                if way in sent:
                    first += (number(sent[way]) + 1) * FIELD ** (way + 1)
            second = sum(number(x) * FIELD**k for k, x in enumerate(pieces))
            third = op + 16 * sum(acc * 4**k for k, acc in enumerate(accs))
            words.append((first, second, third))
        words += [(0, 0, 0)] * (length - len(words))
        packed_tables.append(words)
    return length, packed_tables


def kernel(
    n, groups, per_group, length, tables,
    table_ref, turns_ref, freq_ref, q_hbm, stored_ref, keys_hbm, values_hbm,
    out_ref, paged_ref,
    rows_ref, q_ref, guest_q, guest_turns, cos_ref, sin_ref, held, turned, top, total, raw,
    back, back_stats, came, came_stats, own_sem, send_sem, recv_sem, side_send, side_recv,
):
    me = lax.axis_index("seq")
    partner = me + 1 - 2 * (me % 2)
    tokens = q_hbm.shape[0]
    heads = groups * per_group
    blocks = tokens // QBLK
    scale = HEAD_SIZE ** -0.5 * math.log2(math.e)
    has_right = me + 2 < n
    has_left = me - 2 >= 0
    is_top = me >= n - 2
    is_helper = (me >= n - 4) & (me < n - 2)
    width = per_group * HEAD_SIZE

    def at(j, part, g):
        return (j * KINDS + part) * groups + g

    own = [pltpu.make_async_copy(q_hbm, q_ref, own_sem.at[0])]
    for part in range(PRIOR_SEGMENTS):
        for g in range(groups):
            own.append(
                pltpu.make_async_copy(
                    stored_ref.at[part, g], held.at[at(me, part, g)], own_sem.at[len(own)]
                )
            )
    for g in range(groups):
        for kv, ref in enumerate((keys_hbm, values_hbm)):
            own.append(
                pltpu.make_async_copy(
                    ref.at[:, pl.ds(g * HEAD_SIZE, HEAD_SIZE)],
                    held.at[at(me, CURRENT, g), kv],
                    own_sem.at[len(own)],
                )
            )
    for copy in own:
        copy.start()
    barrier = pltpu.get_barrier_semaphore()
    pl.semaphore_signal(barrier, inc=1, device_id={"seq": partner}, device_id_type=MESH)

    @pl.when(has_right)
    def _():
        pl.semaphore_signal(barrier, inc=1, device_id={"seq": me + 2}, device_id_type=MESH)

    @pl.when(has_left)
    def _():
        pl.semaphore_signal(barrier, inc=1, device_id={"seq": me - 2}, device_id_type=MESH)

    for d in range(n):

        @pl.when(me == d)
        def _():
            for k, words in enumerate(tables[d]):
                rows_ref[0, k] = words[0]
                rows_ref[1, k] = words[2]

    expected = 1 + has_right.astype(jnp.int32) + has_left.astype(jnp.int32)
    pl.semaphore_wait(barrier, expected)

    def side(index, source, destination, target):
        return pltpu.make_async_remote_copy(
            src_ref=source,
            dst_ref=destination,
            send_sem=side_send.at[index],
            recv_sem=side_recv.at[index],
            device_id={"seq": target},
            device_id_type=MESH,
        )

    down = jnp.maximum(me - 2, 0)
    up = jnp.minimum(me + 2, n - 1)
    send_q = side(0, q_ref.at[:, pl.ds(0, width)], guest_q, down)
    send_turns = side(1, turns_ref, guest_turns, down)
    send_back = side(2, back, came, up)
    send_stats = side(3, back_stats, came_stats, up)

    own[0].wait()

    @pl.when(is_top)
    def _():
        send_turns.start()
        send_q.start()

    for copy in own[1:]:
        copy.wait()

    def remote(way, piece):
        target = (me + 2, me - 2, partner)[way]
        return pltpu.make_async_remote_copy(
            src_ref=held.at[piece],
            dst_ref=held.at[piece],
            send_sem=send_sem.at[way, piece],
            recv_sem=recv_sem.at[piece],
            device_id={"seq": target},
            device_id_type=MESH,
        )

    def fields(row):
        word = rows_ref[0, row]
        return [word // FIELD**k % FIELD for k in range(4)]

    def tables_of(ref):
        rows = lax.broadcasted_iota(jnp.int32, (QBLK, HEAD_SIZE), 0).astype(jnp.float32)
        angle = rows * freq_ref[...]
        near_cos, near_sin = jnp.cos(angle), jnp.sin(angle)
        far = ref[...]
        far_cos, far_sin = jnp.cos(far), jnp.sin(far)
        lane = lax.broadcasted_iota(jnp.int32, (QBLK, HEAD_SIZE), 1)
        for part in range(KINDS):
            for b in range(blocks):
                r = part * blocks + b
                c, s = far_cos[r : r + 1], far_sin[r : r + 1]
                span = slice(b * QBLK, (b + 1) * QBLK)
                cos_ref[part, span] = c * near_cos - s * near_sin
                sin = s * near_cos + c * near_sin
                sin_ref[part, span] = jnp.where(lane < HEAD_SIZE // 2, -sin, sin)

    def turn(source, count, base):
        def one(part, carry):
            cos = cos_ref[part]
            sin = sin_ref[part]
            for h in range(count):
                x = source[:, h * HEAD_SIZE : (h + 1) * HEAD_SIZE].astype(jnp.float32)
                y = x * cos + pltpu.roll(x, HEAD_SIZE // 2, 1) * sin
                y = y.astype(jnp.bfloat16).astype(jnp.float32) * scale
                high = y.astype(jnp.bfloat16)
                low = (y - high.astype(jnp.float32)).astype(jnp.bfloat16)
                turned[part, base + h, :HEAD_SIZE] = high.T
                turned[part, base + h, HEAD_SIZE:] = low.T
            return carry

        lax.fori_loop(0, KINDS, one, 0)

    top[...] = jnp.full(top.shape, masked_value, jnp.float32)

    def clear(h, carry):
        total[h] = jnp.zeros(total.shape[1:], jnp.float32)
        return carry

    lax.fori_loop(0, total.shape[0], clear, 0)

    def absorb(streams, causal=False):
        ready = []
        for pieces, base, query in streams:
            keys = []
            for piece in pieces:
                k = held[piece, 0]
                keys.append((jnp.concatenate([k, k], 1), piece // groups % KINDS))
            values = jnp.concatenate([held[piece, 1] for piece in pieces], 0).T
            ones = jnp.ones((ONES_ROWS, values.shape[1]), jnp.bfloat16)
            ready.append((keys, jnp.concatenate([values, ones], 0), base, query))
        units = [(stream, h) for stream in ready for h in range(per_group)]

        def score(unit):
            (keys, _, _, query), h = unit
            some = [
                jnp.dot(k, turned[part, query + h], preferred_element_type=jnp.float32)
                for k, part in keys
            ]
            return some[0] if len(some) == 1 else jnp.concatenate(some, 0)

        def add(unit, weights, factor):
            (_, values, base, _), h = unit
            total[base + h] = total[base + h] * factor + jnp.dot(
                values, weights, preferred_element_type=jnp.float32
            )

        pending = []
        following = score(units[0])
        for k, unit in enumerate(units):
            scores = following
            if k + 1 < len(units):
                following = score(units[k + 1])
            if causal:
                key_index = lax.broadcasted_iota(jnp.int32, scores.shape, 0)
                row_index = lax.broadcasted_iota(jnp.int32, scores.shape, 1)
                scores = jnp.where(key_index <= row_index, scores, masked_value)
            (_, _, base, _), h = unit
            old = top[base + h]
            new = jnp.maximum(old, jnp.max(scores, 0, keepdims=True))
            factor = jnp.exp2(old - new)
            weights = jnp.exp2(scores - new).astype(jnp.bfloat16)
            top[base + h] = new
            if len(pending) == 2:
                add(*pending.pop(0))
            pending.append((unit, weights, factor))
        for some in pending:
            add(*some)

    rounds = tokens // PAGE_TOKENS // n
    here = n * rounds
    last = PRIOR_SEGMENTS - 1

    def pages():
        def collect(j, carry):
            for r in range(rounds):
                rows = pl.ds(pl.multiple_of((r * n + me) * PAGE_TOKENS, PAGE_TOKENS), PAGE_TOKENS)
                to = pl.ds(pl.multiple_of((j * rounds + r) * PAGE_TOKENS, PAGE_TOKENS), PAGE_TOKENS)
                for kv in range(2):
                    for g in range(groups):
                        raw[kv, to, g * HEAD_SIZE : (g + 1) * HEAD_SIZE] = held[
                            at(j, last, g), kv, rows, :
                        ]
            return carry

        lax.fori_loop(0, n, collect, 0)
        size = here * PAGE_TOKENS
        row = lax.broadcasted_iota(jnp.int32, (size, size), 0)
        column = lax.broadcasted_iota(jnp.int32, (size, size), 1)
        slot = lax.broadcasted_iota(jnp.int32, (1, size), 1) // PAGE_TOKENS
        page = jnp.zeros((1, size), jnp.int32)
        for k in range(here):
            j, r = k // rounds, k % rounds
            entry = table_ref[j * (tokens // PAGE_TOKENS) + r * n + me]
            page = jnp.where(slot == k, entry, page)
        chosen = (row % here == page) & (row // here == column % PAGE_TOKENS)
        pick = jnp.where(chosen, 1.0, 0.0).astype(jnp.bfloat16)
        for kv in range(2):
            moved = jnp.dot(pick, raw[kv], preferred_element_type=jnp.float32)
            moved = moved.astype(jnp.bfloat16)
            for g in range(groups):
                for t in range(PAGE_TOKENS):
                    paged_ref[kv, g, :, t * HEAD_SIZE : (t + 1) * HEAD_SIZE] = moved[
                        t * here : (t + 1) * here, g * HEAD_SIZE : (g + 1) * HEAD_SIZE
                    ]

    guest_base = heads
    spare_base = heads + per_group

    def step(row, carry):
        wait, *sent = fields(row)

        @pl.when(wait > 0)
        def _():
            remote(RIGHT, wait - 1).wait_recv()

        for way in (ACROSS, RIGHT, LEFT):

            @pl.when(sent[way] > 0)
            def _():
                remote(way, sent[way] - 1).start()

        third = rows_ref[1, row]
        op = third % 16

        def listed():
            word = jnp.int32(0)
            for r in range(length):
                choice = None
                for d in range(n):
                    value = tables[d][r][1]
                    if value:
                        choice = value if choice is None else jnp.where(me == d, value, choice)
                if choice is not None:
                    word = jnp.where(row == r, choice, word)
            return word

        def stream(k, size, second):
            acc = third // (16 * 4**k) % 4
            pieces = [second // FIELD ** (k * size + i) % FIELD for i in range(size)]
            base = acc * per_group
            query = jnp.where(acc == SPARE, 0, base)
            return pieces, base, query

        @pl.when(op == BATCH2)
        def _():
            word = listed()
            absorb([stream(0, 2, word), stream(1, 2, word)])

        @pl.when(op == BATCH1)
        def _():
            word = listed()
            absorb([stream(0, 1, word), stream(1, 1, word)])

        @pl.when(op == TURN)
        def _():
            tables_of(turns_ref)
            turn(q_ref, heads, 0)

        @pl.when(op == DIAGONAL)
        def _():
            absorb(
                [([at(me, CURRENT, g)], g * per_group, g * per_group) for g in range(groups)], True
            )

        @pl.when(op == GUEST_TURN)
        def _():
            send_turns.wait_recv()
            send_q.wait_recv()
            tables_of(guest_turns)
            turn(guest_q, per_group, guest_base)

        @pl.when(op == PACK)
        def _():
            for h in range(per_group):
                part = total[guest_base + h]
                share = part[HEAD_SIZE : HEAD_SIZE + 1]
                back[h] = (part[:HEAD_SIZE] / share).astype(jnp.bfloat16)
                back_stats[0, h : h + 1] = top[guest_base + h]
                back_stats[1, h : h + 1] = share

        @pl.when(op == RETURN)
        def _():
            send_stats.start()
            send_back.start()

        @pl.when(op == PAGES)
        def _():
            pages()

        @pl.when(op == MERGE)
        def _():
            send_stats.wait_recv()
            send_back.wait_recv()
            for h in range(per_group):
                mine, other = top[h], came_stats[0, h : h + 1]
                new = jnp.maximum(mine, other)
                keep = jnp.exp2(mine - new)
                share = came_stats[1, h : h + 1] * jnp.exp2(other - new)
                total[h, :HEAD_SIZE] = (
                    total[h, :HEAD_SIZE] * keep + came[h].astype(jnp.float32) * share
                )
                total[h, HEAD_SIZE : HEAD_SIZE + 1] = (
                    total[h, HEAD_SIZE : HEAD_SIZE + 1] * keep + share
                )

        return carry

    lax.fori_loop(0, length, step, 0)

    for h in range(heads):
        finished = total[h, :HEAD_SIZE] / total[h, HEAD_SIZE : HEAD_SIZE + 1]
        out_ref[:, h * HEAD_SIZE : (h + 1) * HEAD_SIZE] = finished.T.astype(out_ref.dtype)

    def drain(row, carry):
        _, *sent = fields(row)
        for way in (ACROSS, RIGHT, LEFT):

            @pl.when(sent[way] > 0)
            def _():
                remote(way, sent[way] - 1).wait_send()

        return carry

    lax.fori_loop(0, length, drain, 0)

    @pl.when(is_top)
    def _():
        send_turns.wait_send()
        send_q.wait_send()

    @pl.when(is_helper)
    def _():
        send_stats.wait_send()
        send_back.wait_send()


def shards(
    queries, current_keys, current_values, stored_keys, stored_values, remap_table, block_table
):
    tokens, width = queries.shape
    key_width = current_keys.shape[1]
    groups = key_width // HEAD_SIZE
    heads = width // HEAD_SIZE
    per_group = heads // groups
    owners = lax.axis_size("seq")
    length, tables = schedule(owners, groups)
    pieces = owners * KINDS * groups
    blocks = tokens // QBLK
    half_dim = HEAD_SIZE // 2
    frequency = rope_base ** (-2.0 * jnp.arange(half_dim, dtype=jnp.float32) / HEAD_SIZE)
    frequency = jnp.concatenate([frequency, frequency])[None, :]
    bases = remap_table[::-1].reshape(KINDS * blocks, 1).astype(jnp.float32)
    turns = jnp.pad(bases * frequency, ((0, -KINDS * blocks % 8), (0, 0)))
    stored = jnp.stack(
        [
            jnp.stack(
                [
                    jnp.stack([x[:, s, g * HEAD_SIZE : (g + 1) * HEAD_SIZE] for x in (stored_keys, stored_values)])
                    for g in range(groups)
                ]
            )
            for s in range(PRIOR_SEGMENTS)
        ]
    )
    rounds = tokens // PAGE_TOKENS // owners
    here = owners * rounds
    hbm = pl.BlockSpec(memory_space=pltpu.HBM)
    vmem = pl.BlockSpec(memory_space=pltpu.VMEM)
    smem = pl.BlockSpec(memory_space=pltpu.SMEM)
    slots = heads + 2 * per_group
    bf16, f32 = jnp.bfloat16, jnp.float32
    attended, paged = pl.pallas_call(
        functools.partial(kernel, owners, groups, per_group, length, tables),
        out_shape=(
            jax.ShapeDtypeStruct((tokens, width), bf16),
            jax.ShapeDtypeStruct((2, groups, here, PAGE_TOKENS * HEAD_SIZE), bf16),
        ),
        in_specs=[smem, vmem, vmem, hbm, hbm, hbm, hbm],
        out_specs=(vmem, vmem),
        scratch_shapes=[
            pltpu.SMEM((2, length), jnp.int32),
            pltpu.VMEM((tokens, width), bf16),
            pltpu.VMEM((tokens, per_group * HEAD_SIZE), bf16),
            pltpu.VMEM(turns.shape, f32),
            pltpu.VMEM((KINDS, tokens, HEAD_SIZE), f32),
            pltpu.VMEM((KINDS, tokens, HEAD_SIZE), f32),
            pltpu.VMEM((pieces, 2, tokens, HEAD_SIZE), bf16),
            pltpu.VMEM((KINDS, heads + per_group, 2 * HEAD_SIZE, tokens), bf16),
            pltpu.VMEM((slots, 1, tokens), f32),
            pltpu.VMEM((slots, HEAD_SIZE + ONES_ROWS, tokens), f32),
            pltpu.VMEM((2, here * PAGE_TOKENS, key_width), bf16),
            pltpu.VMEM((per_group, HEAD_SIZE, tokens), bf16),
            pltpu.VMEM((2, per_group, tokens), f32),
            pltpu.VMEM((per_group, HEAD_SIZE, tokens), bf16),
            pltpu.VMEM((2, per_group, tokens), f32),
            pltpu.SemaphoreType.DMA((1 + PRIOR_SEGMENTS * groups + 2 * groups,)),
            pltpu.SemaphoreType.DMA((3, pieces)),
            pltpu.SemaphoreType.DMA((pieces,)),
            pltpu.SemaphoreType.DMA((4,)),
            pltpu.SemaphoreType.DMA((4,)),
        ],
        compiler_params=pltpu.CompilerParams(
            collective_id=0, has_side_effects=True, vmem_limit_bytes=56 * 1024 * 1024
        ),
    )(block_table, turns, frequency, queries, stored, current_keys, current_values)
    return (attended, paged[0], paged[1])


def solution(mesh):
    in_specs = (
        P(("groups", "seq"), "head"),
        P(("groups", "seq"), "head"),
        P(("groups", "seq"), "head"),
        P(("groups", "seq"), None, "head"),
        P(("groups", "seq"), None, "head"),
        P(None, ("groups", "seq")),
        P("groups"),
    )
    out_specs = (
        P(("groups", "seq"), "head"),
        P("head", ("groups", "seq"), None),
        P("head", ("groups", "seq"), None),
    )
    return jax.shard_map(shards, mesh=mesh, in_specs=in_specs, out_specs=out_specs, check_vma=False)
```

```python
import functools
import heapq
import math

import jax
import jax.numpy as jnp
from jax import lax
from jax.experimental import pallas as pl
from jax.experimental.pallas import tpu as pltpu
from jax.sharding import PartitionSpec as P

HEAD_SIZE = 128
PRIOR_SEGMENTS = 2
PAGE_TOKENS = 16
QBLK = 64
KINDS = PRIOR_SEGMENTS + 1
CURRENT = PRIOR_SEGMENTS

rope_base = 1000000.0
masked_value = -1e30
MESH = pl.DeviceIdType.MESH
RIGHT, LEFT, ACROSS = 0, 1, 2
ONES_ROWS = 16
GRANT = 40 * 1024 * 1024

OWN0, OWN1, GUEST, SPARE = 0, 1, 2, 3
NOTHING, BATCH2, BATCH1, TURN, DIAGONAL, GUEST_TURN, PACK, RETURN, PAGES, MERGE = range(10)
FIELD = 128

WIRE, HOP, RELAY = 2.81, 1.9, 1.0
COST = {BATCH2: 2.6, BATCH1: 1.5, TURN: 4.0, DIAGONAL: 1.6, GUEST_TURN: 2.0, PACK: 0.8, PAGES: 1.3}


def offloaded(n, d):
    if d < n - 2 or n < 4:
        return set()
    return {
        (j, part, 0)
        for j in range(n - 2)
        for part in (0, CURRENT)
        if part < CURRENT or j <= n - 4
    }


def needed(n, groups, d):
    left = offloaded(n, d)
    return {
        (j, part, g)
        for j in range(n)
        for part in range(KINDS)
        for g in range(groups)
        if j != d and (part < CURRENT or j < d) and (j, part, g) not in left
    }


def route(n, groups):
    need = {d: needed(n, groups, d) for d in range(n)}
    here = {
        d: {(d, part, g): 0.0 for part in range(KINDS) for g in range(groups)} for d in range(n)
    }
    taken = {d: set(here[d]) for d in range(n)}
    lack = {}
    for d in range(n):
        for x in sorted(need[d]):
            lack[x] = lack.get(x, 0) + 1
    target = {}
    for d in range(n):
        if d + 2 < n:
            target[(d, RIGHT)] = d + 2
        if d - 2 >= 0:
            target[(d, LEFT)] = d - 2
        target[(d, ACROSS)] = d ^ 1
    wanted = {d - 2: offloaded(n, d) for d in range(n) if offloaded(n, d)}
    urgent = set().union(*wanted.values()) if wanted else set()
    free = {link: 0.0 for link in target}
    for h in wanted:
        free[(h + 2, LEFT)] = 3.5 * WIRE
    ready = {}
    returned = {}
    sends = {link: [] for link in target}
    arrivals = {d: {} for d in range(n)}
    events = []
    for k, link in enumerate(target):
        heapq.heappush(events, (free[link], k, 0, link))
    count = len(events)
    idle = set()

    def pick(link, now):
        u, v = link[0], target[link]
        if link[1] == RIGHT and u in wanted and u not in returned and ready.get(u, now + 1) <= now:
            return RETURN
        best = None
        for x in sorted(here[u]):
            if here[u][x] > now + 1e-9 or x in taken[v] or x not in need[v]:
                continue
            others = sum(1 for w in (v + 2, v - 2, v ^ 1) if 0 <= w < n and w != u and x in taken[w])
            score = lack[x] - SHARED * others
            if x in urgent and (v in wanted or (link[1] != LEFT and v < n - 4)):
                score += BONUS
            score += ((x[0] * 7 + x[1] * 5 + x[2] * 3 + u * 11 + link[1] * 13 + SALT) * 7919 % 101) / 101
            if best is None or score > best[0]:
                best = (score, x)
        return None if best is None else best[1]

    while events:
        now, _, kind, what = heapq.heappop(events)
        if kind == 0:
            link = what
            if free[link] > now + 1e-9:
                heapq.heappush(events, (free[link], count, 0, link))
                count += 1
                continue
            x = pick(link, now)
            if x is None:
                idle.add(link)
                continue
            v = target[link]
            if x == RETURN:
                returned[link[0]] = now + 3.6 * WIRE + HOP
                free[link] = now + 3.6 * WIRE
            else:
                taken[v].add(x)
                lack[x] -= 1
                sends[link].append(x)
                arrivals[v][x] = now + WIRE + HOP
                here[v][x] = now + WIRE + HOP + RELAY
                free[link] = now + WIRE
                heapq.heappush(events, (here[v][x], count, 1, v))
                count += 1
                if v in wanted and v not in ready and wanted[v] <= set(here[v]):
                    ready[v] = max(here[v][y] for y in wanted[v]) + 4.0
                    heapq.heappush(events, (ready[v], count, 1, v))
                    count += 1
            heapq.heappush(events, (free[link], count, 0, link))
            count += 1
        else:
            for link in sorted(x for x in idle if x[0] == what):
                idle.discard(link)
                heapq.heappush(events, (max(now, free[link]), count, 0, link))
                count += 1
    return sends, arrivals, wanted, returned


SALT, BONUS, SHARED = 16, 3.0, 2.0


def schedule(n, groups):
    sends, arrivals, wanted, returned = route(n, groups)
    tables = []
    for d in range(n):
        rows = []
        have = {(d, part, g) for part in range(KINDS) for g in range(groups)}
        queue = {way: list(sends.get((d, way), [])) for way in (RIGHT, LEFT, ACROSS)}
        order = sorted(arrivals[d], key=lambda x: (arrivals[d][x], x))
        guest = sorted(wanted.get(d, ()))
        pending = {OWN0: [], OWN1: [], GUEST: []}
        absorbed_guest = 0
        turned_guest = packed = sent_back = paged = False
        pages_left = {(j, 1, g) for j in range(n) for g in range(groups)} - have

        def ready_sends():
            out = {}
            for way, q in queue.items():
                if q and q[0] in have:
                    out[way] = q.pop(0)
            return out

        def emit(wait=None, op=NOTHING, pieces=(), accs=()):
            if wait is not None:
                have.add(wait)
            if wait is None and op != NOTHING and rows and rows[-1][2] == NOTHING:
                rows[-1][2:] = [op, list(pieces), list(accs)]
                return
            rows.append([wait, ready_sends(), op, list(pieces), list(accs)])
            while True:
                more = ready_sends()
                if not more:
                    break
                rows.append([None, more, NOTHING, [], []])

        def note(x):
            pages_left.discard(x)
            pending[x[2]].append(x)
            if x in guest:
                pending[GUEST].append(x)

        def streams(count, size):
            chosen = []
            for acc in (GUEST, OWN0, OWN1):
                if acc == GUEST and not turned_guest:
                    continue
                while len(pending[acc]) >= size and len(chosen) < count:
                    chosen.append((acc, [pending[acc].pop(0) for _ in range(size)]))
            return chosen

        def put_back(chosen):
            for acc, pieces in reversed(chosen):
                pending[acc] = pieces + pending[acc]

        def batch(op, chosen):
            nonlocal now, absorbed_guest
            pieces, accs = [], []
            for acc, some in chosen:
                pieces += some
                accs.append(acc)
                absorbed_guest += len(some) if acc == GUEST else 0
            emit(None, op, pieces, accs)
            now += COST[op]

        emit()
        emit(None, TURN)
        now = COST[TURN]
        for g in range(groups):
            for part in range(PRIOR_SEGMENTS):
                note((d, part, g))
            if (d, CURRENT, g) in guest:
                pending[GUEST].append((d, CURRENT, g))
        first = [(OWN0, [pending[OWN0].pop(0) for _ in range(2)]),
                 (OWN1, [pending[OWN1].pop(0) for _ in range(2)])]
        batch(BATCH2, first)
        emit(None, DIAGONAL)
        now += COST[DIAGONAL]
        guest_at = 3.5 * WIRE + HOP + 1.0
        while True:
            while order and arrivals[d][order[0]] <= now + 0.2:
                x = order.pop(0)
                emit(x)
                note(x)
            if guest and not turned_guest and guest_at <= now:
                emit(None, GUEST_TURN)
                now += COST[GUEST_TURN]
                turned_guest = True
                continue
            if packed and not sent_back:
                emit(None, RETURN)
                sent_back = True
                continue
            if guest and not packed and absorbed_guest == len(guest):
                emit(None, PACK)
                now += COST[PACK]
                packed = True
                continue
            chosen = streams(2, 2)
            if len(chosen) == 2:
                batch(BATCH2, chosen)
                continue
            put_back(chosen)
            last_guest = (
                guest and turned_guest and absorbed_guest + len(pending[GUEST]) == len(guest)
            )
            upcoming = arrivals[d][order[0]] if order else None
            if last_guest and pending[GUEST]:
                chosen = streams(2, 1)
                if len(chosen) == 1:
                    chosen.append((SPARE, list(chosen[0][1])))
                batch(BATCH1, chosen)
                continue
            if not pages_left and not paged:
                emit(None, PAGES)
                now += COST[PAGES]
                paged = True
                continue
            if guest and not turned_guest and (upcoming is None or guest_at <= upcoming):
                now = max(now, guest_at)
                continue
            if upcoming is None or upcoming - now > 1.2:
                chosen = streams(2, 1)
                if len(chosen) == 2:
                    batch(BATCH1, chosen)
                    continue
                if chosen and upcoming is None:
                    chosen.append((SPARE, list(chosen[0][1])))
                    batch(BATCH1, chosen)
                    continue
                put_back(chosen)
            if upcoming is None:
                break
            now = max(now, upcoming)
        if offloaded(n, d):
            emit(None, MERGE)
        assert not any(queue.values()) and not any(pending.values()) and paged
        tables.append(rows)
    length = max(len(rows) for rows in tables)

    def number(x):
        return (x[0] * KINDS + x[1]) * groups + x[2]

    packed_tables = []
    for rows in tables:
        words = []
        for wait, sent, op, pieces, accs in rows:
            first = [0 if wait is None else number(wait) + 1]
            first += [number(sent[way]) + 1 if way in sent else 0 for way in (RIGHT, LEFT, ACROSS)]
            listed = sum(number(x) * FIELD**k for k, x in enumerate(pieces))
            accs = list(accs) + [0] * (2 - len(accs))
            words.append((first + [op] + accs, listed))
        words += [([0] * 7, 0)] * (length - len(words))
        packed_tables.append(words)
    return length, packed_tables


def kernel(n, groups, per_group, length, tables, table_ref, remap_ref, q_hbm, *refs):
    sources = [refs[2 * part : 2 * part + 2] for part in range(KINDS)]
    (
        out_ref, paged_keys_ref, paged_values_ref,
        rows_ref, q_ref, turns, guest_q, guest_turns, cos_ref, sin_ref, held, turned, top, total,
        raw, back, back_stats, came, came_stats, own_sem, send_sem, recv_sem, side_send, side_recv,
    ) = refs[2 * KINDS :]
    me = lax.axis_index("seq")
    partner = me + 1 - 2 * (me % 2)
    tokens = q_hbm.shape[0]
    heads = groups * per_group
    blocks = tokens // QBLK
    scale = HEAD_SIZE ** -0.5 * math.log2(math.e)
    has_right = me + 2 < n
    has_left = me - 2 >= 0
    is_top = me >= n - 2
    is_helper = (me >= n - 4) & (me < n - 2)
    width = per_group * HEAD_SIZE

    def at(j, part, g):
        return (j * KINDS + part) * groups + g

    own = [pltpu.make_async_copy(q_hbm, q_ref, own_sem.at[0])]
    for part in range(KINDS):
        for g in range(groups):
            for kv, ref in enumerate(sources[part]):
                own.append(
                    pltpu.make_async_copy(
                        ref.at[:, pl.ds(g * HEAD_SIZE, HEAD_SIZE)],
                        held.at[at(me, part, g), kv],
                        own_sem.at[len(own)],
                    )
                )
    for copy in own:
        copy.start()
    barrier = pltpu.get_barrier_semaphore()
    pl.semaphore_signal(barrier, inc=1, device_id={"seq": partner}, device_id_type=MESH)

    @pl.when(has_right)
    def _():
        pl.semaphore_signal(barrier, inc=1, device_id={"seq": me + 2}, device_id_type=MESH)

    @pl.when(has_left)
    def _():
        pl.semaphore_signal(barrier, inc=1, device_id={"seq": me - 2}, device_id_type=MESH)

    lane = lax.broadcasted_iota(jnp.int32, (1, HEAD_SIZE), 1)
    power = (lane % (HEAD_SIZE // 2)).astype(jnp.float32) * (-2.0 * math.log2(rope_base) / HEAD_SIZE)
    frequency = jnp.exp2(power)
    for part in range(KINDS):
        for b in range(blocks):
            base = remap_ref[KINDS - 1 - part, b].astype(jnp.float32)
            turns[part * blocks + b : part * blocks + b + 1] = base * frequency
    if turns.shape[0] > KINDS * blocks:
        rest = turns.shape[0] - KINDS * blocks
        turns[KINDS * blocks :] = jnp.zeros((rest, HEAD_SIZE), jnp.float32)

    for d in range(n):

        @pl.when(me == d)
        def _():
            for k, (words, _) in enumerate(tables[d]):
                for c, word in enumerate(words):
                    rows_ref[c, k] = word * per_group if c > 4 else word

    top[...] = jnp.full(top.shape, masked_value, jnp.float32)

    def clear(h, carry):
        total[h] = jnp.zeros(total.shape[1:], jnp.float32)
        return carry

    lax.fori_loop(0, total.shape[0], clear, 0)

    expected = 1 + has_right.astype(jnp.int32) + has_left.astype(jnp.int32)
    pl.semaphore_wait(barrier, expected)

    def side(index, source, destination, target):
        return pltpu.make_async_remote_copy(
            src_ref=source,
            dst_ref=destination,
            send_sem=side_send.at[index],
            recv_sem=side_recv.at[index],
            device_id={"seq": target},
            device_id_type=MESH,
        )

    down = jnp.maximum(me - 2, 0)
    up = jnp.minimum(me + 2, n - 1)
    send_q = side(0, q_ref.at[:, pl.ds(0, width)], guest_q, down)
    send_turns = side(1, turns, guest_turns, down)
    send_back = side(2, back, came, up)
    send_stats = side(3, back_stats, came_stats, up)

    own[0].wait()

    @pl.when(is_top)
    def _():
        send_turns.start()
        send_q.start()

    for copy in own[1:]:
        copy.wait()

    def remote(way, piece):
        target = (me + 2, me - 2, partner)[way]
        return pltpu.make_async_remote_copy(
            src_ref=held.at[piece],
            dst_ref=held.at[piece],
            send_sem=send_sem.at[way, piece],
            recv_sem=recv_sem.at[piece],
            device_id={"seq": target},
            device_id_type=MESH,
        )

    def tables_of(ref):
        rows = lax.broadcasted_iota(jnp.int32, (QBLK, HEAD_SIZE), 0).astype(jnp.float32)
        angle = rows * frequency
        near_cos, near_sin = jnp.cos(angle), jnp.sin(angle)
        far = ref[...]
        far_cos, far_sin = jnp.cos(far), jnp.sin(far)
        lane = lax.broadcasted_iota(jnp.int32, (QBLK, HEAD_SIZE), 1)
        for part in range(KINDS):
            for b in range(blocks):
                r = part * blocks + b
                c, s = far_cos[r : r + 1], far_sin[r : r + 1]
                span = slice(b * QBLK, (b + 1) * QBLK)
                cos_ref[part, span] = c * near_cos - s * near_sin
                sin = s * near_cos + c * near_sin
                sin_ref[part, span] = jnp.where(lane < HEAD_SIZE // 2, -sin, sin)

    def turn(source, count, base):
        def one(part, carry):
            cos = cos_ref[part]
            sin = sin_ref[part]
            for h in range(count):
                x = source[:, h * HEAD_SIZE : (h + 1) * HEAD_SIZE].astype(jnp.float32)
                y = x * cos + pltpu.roll(x, HEAD_SIZE // 2, 1) * sin
                y = y.astype(jnp.bfloat16).astype(jnp.float32) * scale
                high = y.astype(jnp.bfloat16)
                low = (y - high.astype(jnp.float32)).astype(jnp.bfloat16)
                turned[part, base + h, :HEAD_SIZE] = high.T
                turned[part, base + h, HEAD_SIZE:] = low.T
            return carry

        lax.fori_loop(0, KINDS, one, 0)

    def absorb(streams, causal=False):
        ready = []
        for pieces, base, query in streams:
            keys = []
            for piece in pieces:
                k = held[piece, 0]
                keys.append((jnp.concatenate([k, k], 1), piece // groups % KINDS))
            values = jnp.concatenate([held[piece, 1] for piece in pieces], 0).T
            ones = jnp.ones((ONES_ROWS, values.shape[1]), jnp.bfloat16)
            ready.append((keys, jnp.concatenate([values, ones], 0), base, query))
        units = [(stream, h) for stream in ready for h in range(per_group)]

        def score(unit):
            (keys, _, _, query), h = unit
            some = [
                jnp.dot(k, turned[part, query + h], preferred_element_type=jnp.float32)
                for k, part in keys
            ]
            return some[0] if len(some) == 1 else jnp.concatenate(some, 0)

        def add(unit, weights, factor):
            (_, values, base, _), h = unit
            total[base + h] = total[base + h] * factor + jnp.dot(
                values, weights, preferred_element_type=jnp.float32
            )

        pending = []
        following = score(units[0])
        for k, unit in enumerate(units):
            scores = following
            if k + 1 < len(units):
                following = score(units[k + 1])
            if causal:
                key_index = lax.broadcasted_iota(jnp.int32, scores.shape, 0)
                row_index = lax.broadcasted_iota(jnp.int32, scores.shape, 1)
                scores = jnp.where(key_index <= row_index, scores, masked_value)
            (_, _, base, _), h = unit
            old = top[base + h]
            new = jnp.maximum(old, jnp.max(scores, 0, keepdims=True))
            factor = jnp.exp2(old - new)
            weights = jnp.exp2(scores - new).astype(jnp.bfloat16)
            top[base + h] = new
            if len(pending) == 2:
                add(*pending.pop(0))
            pending.append((unit, weights, factor))
        for some in pending:
            add(*some)

    rounds = tokens // PAGE_TOKENS // n
    here = n * rounds
    last = PRIOR_SEGMENTS - 1

    def pages():
        def collect(j, carry):
            for r in range(rounds):
                rows = pl.ds(pl.multiple_of((r * n + me) * PAGE_TOKENS, PAGE_TOKENS), PAGE_TOKENS)
                to = pl.ds(pl.multiple_of((j * rounds + r) * PAGE_TOKENS, PAGE_TOKENS), PAGE_TOKENS)
                for kv in range(2):
                    for g in range(groups):
                        raw[kv, to, g * HEAD_SIZE : (g + 1) * HEAD_SIZE] = held[
                            at(j, last, g), kv, rows, :
                        ]
            return carry

        lax.fori_loop(0, n, collect, 0)
        size = here * PAGE_TOKENS
        row = lax.broadcasted_iota(jnp.int32, (size, size), 0)
        column = lax.broadcasted_iota(jnp.int32, (size, size), 1)
        slot = lax.broadcasted_iota(jnp.int32, (1, size), 1) // PAGE_TOKENS
        page = jnp.zeros((1, size), jnp.int32)
        for k in range(here):
            j, r = k // rounds, k % rounds
            entry = table_ref[j * (tokens // PAGE_TOKENS) + r * n + me]
            page = jnp.where(slot == k, entry, page)
        chosen = (row % here == page) & (row // here == column % PAGE_TOKENS)
        pick = jnp.where(chosen, 1.0, 0.0).astype(jnp.bfloat16)
        for kv in range(2):
            moved = jnp.dot(pick, raw[kv], preferred_element_type=jnp.float32)
            moved = moved.astype(jnp.bfloat16)
            for g in range(groups):
                for t in range(PAGE_TOKENS):
                    (paged_keys_ref, paged_values_ref)[kv][g, :, t * HEAD_SIZE : (t + 1) * HEAD_SIZE] = moved[
                        t * here : (t + 1) * here, g * HEAD_SIZE : (g + 1) * HEAD_SIZE
                    ]

    guest_base = heads
    spare_base = heads + per_group

    listed = []
    for r in range(length):
        choice = None
        for d in range(n):
            value = tables[d][r][1]
            if value:
                choice = value if choice is None else jnp.where(me == d, value, choice)
        if choice is not None:
            listed.append((r, choice))

    def step(row, carry):
        wait, right, left, across, op, first, second = [rows_ref[c, row] for c in range(7)]

        @pl.when(wait > 0)
        def _():
            remote(RIGHT, wait - 1).wait_recv()

        @pl.when(right + left + across > 0)
        def _():
            for way, sent in ((ACROSS, across), (RIGHT, right), (LEFT, left)):

                @pl.when(sent > 0)
                def _():
                    remote(way, sent - 1).start()

        def streams(size):
            word = jnp.int32(0)
            for r, choice in listed:
                word = jnp.where(row == r, choice, word)
            some = []
            for k, base in enumerate((first, second)):
                pieces = [word // FIELD ** (k * size + i) % FIELD for i in range(size)]
                some.append((pieces, base, jnp.where(base == spare_base, 0, base)))
            return some

        @pl.when(op == BATCH2)
        def _():
            absorb(streams(2))

        @pl.when(op == BATCH1)
        def _():
            absorb(streams(1))

        @pl.when(op > BATCH1)
        def _():
            others(op)

        return carry

    def others(op):
        @pl.when(op == TURN)
        def _():
            tables_of(turns)
            turn(q_ref, heads, 0)

        @pl.when(op == DIAGONAL)
        def _():
            absorb(
                [([at(me, CURRENT, g)], g * per_group, g * per_group) for g in range(groups)], True
            )

        @pl.when(op == GUEST_TURN)
        def _():
            send_turns.wait_recv()
            send_q.wait_recv()
            tables_of(guest_turns)
            turn(guest_q, per_group, guest_base)

        @pl.when(op == PACK)
        def _():
            for h in range(per_group):
                part = total[guest_base + h]
                share = part[HEAD_SIZE : HEAD_SIZE + 1]
                back[h] = (part[:HEAD_SIZE] / share).astype(jnp.bfloat16)
                back_stats[0, h : h + 1] = top[guest_base + h]
                back_stats[1, h : h + 1] = share

        @pl.when(op == RETURN)
        def _():
            send_stats.start()
            send_back.start()

        @pl.when(op == PAGES)
        def _():
            pages()

        @pl.when(op == MERGE)
        def _():
            send_stats.wait_recv()
            send_back.wait_recv()
            for h in range(per_group):
                mine, other = top[h], came_stats[0, h : h + 1]
                new = jnp.maximum(mine, other)
                keep = jnp.exp2(mine - new)
                share = came_stats[1, h : h + 1] * jnp.exp2(other - new)
                total[h, :HEAD_SIZE] = (
                    total[h, :HEAD_SIZE] * keep + came[h].astype(jnp.float32) * share
                )
                total[h, HEAD_SIZE : HEAD_SIZE + 1] = (
                    total[h, HEAD_SIZE : HEAD_SIZE + 1] * keep + share
                )

    lax.fori_loop(0, length, step, 0)

    for h in range(heads):
        finished = total[h, :HEAD_SIZE] / total[h, HEAD_SIZE : HEAD_SIZE + 1]
        out_ref[:, h * HEAD_SIZE : (h + 1) * HEAD_SIZE] = finished.T.astype(out_ref.dtype)

    for d in range(n):

        @pl.when(me == d)
        def _():
            for words, _ in tables[d]:
                for way in (RIGHT, LEFT, ACROSS):
                    if words[1 + way]:
                        remote(way, words[1 + way] - 1).wait_send()

    @pl.when(is_top)
    def _():
        send_turns.wait_send()
        send_q.wait_send()

    @pl.when(is_helper)
    def _():
        send_stats.wait_send()
        send_back.wait_send()


def finish(*refs):
    half = len(refs) // 3
    copies = [
        pltpu.make_async_copy(refs[k], refs[half + k], refs[2 * half + k]) for k in range(half)
    ]
    for copy in copies:
        copy.start()
    for copy in copies:
        copy.wait()


def shards(
    queries, current_keys, current_values, stored_keys, stored_values, remap_table, block_table
):
    tokens, width = queries.shape
    key_width = current_keys.shape[1]
    groups = key_width // HEAD_SIZE
    heads = width // HEAD_SIZE
    per_group = heads // groups
    owners = lax.axis_size("seq")
    length, tables = schedule(owners, groups)
    pieces = owners * KINDS * groups
    blocks = tokens // QBLK
    sources = [x[:, s, :] for s in range(PRIOR_SEGMENTS) for x in (stored_keys, stored_values)]
    sources += [current_keys, current_values]
    rounds = tokens // PAGE_TOKENS // owners
    here = owners * rounds
    hbm = pl.BlockSpec(memory_space=pltpu.HBM)
    vmem = pl.BlockSpec(memory_space=pltpu.VMEM)
    smem = pl.BlockSpec(memory_space=pltpu.SMEM)
    slots = heads + 2 * per_group
    turn_rows = -(-KINDS * blocks // 8) * 8
    bf16, f32 = jnp.bfloat16, jnp.float32
    results = pl.pallas_call(
        functools.partial(kernel, owners, groups, per_group, length, tables),
        out_shape=(
            jax.ShapeDtypeStruct((tokens, width), bf16),
            jax.ShapeDtypeStruct((groups, here, PAGE_TOKENS * HEAD_SIZE), bf16),
            jax.ShapeDtypeStruct((groups, here, PAGE_TOKENS * HEAD_SIZE), bf16),
        ),
        in_specs=[smem, smem, hbm] + [hbm] * len(sources),
        out_specs=(vmem, vmem, vmem),
        scratch_shapes=[
            pltpu.SMEM((7, length), jnp.int32),
            pltpu.VMEM((tokens, width), bf16),
            pltpu.VMEM((turn_rows, HEAD_SIZE), f32),
            pltpu.VMEM((tokens, per_group * HEAD_SIZE), bf16),
            pltpu.VMEM((turn_rows, HEAD_SIZE), f32),
            pltpu.VMEM((KINDS, tokens, HEAD_SIZE), f32),
            pltpu.VMEM((KINDS, tokens, HEAD_SIZE), f32),
            pltpu.VMEM((pieces, 2, tokens, HEAD_SIZE), bf16),
            pltpu.VMEM((KINDS, heads + per_group, 2 * HEAD_SIZE, tokens), bf16),
            pltpu.VMEM((slots, 1, tokens), f32),
            pltpu.VMEM((slots, HEAD_SIZE + ONES_ROWS, tokens), f32),
            pltpu.VMEM((2, here * PAGE_TOKENS, key_width), bf16),
            pltpu.VMEM((per_group, HEAD_SIZE, tokens), bf16),
            pltpu.VMEM((2, per_group, tokens), f32),
            pltpu.VMEM((per_group, HEAD_SIZE, tokens), bf16),
            pltpu.VMEM((2, per_group, tokens), f32),
            pltpu.SemaphoreType.DMA((1 + 2 * KINDS * groups,)),
            pltpu.SemaphoreType.DMA((3, pieces)),
            pltpu.SemaphoreType.DMA((pieces,)),
            pltpu.SemaphoreType.DMA((4,)),
            pltpu.SemaphoreType.DMA((4,)),
        ],
        compiler_params=pltpu.CompilerParams(
            collective_id=0, has_side_effects=True, vmem_limit_bytes=GRANT
        ),
    )(block_table, remap_table, queries, *sources)
    return pl.pallas_call(
        finish,
        out_shape=tuple(jax.ShapeDtypeStruct(x.shape, x.dtype) for x in results),
        in_specs=[vmem] * 3,
        out_specs=(hbm,) * 3,
        scratch_shapes=[pltpu.SemaphoreType.DMA] * 3,
        compiler_params=pltpu.CompilerParams(vmem_limit_bytes=8 * 1024 * 1024),
    )(*results)


def solution(mesh):
    in_specs = (
        P(("groups", "seq"), "head"),
        P(("groups", "seq"), "head"),
        P(("groups", "seq"), "head"),
        P(("groups", "seq"), None, "head"),
        P(("groups", "seq"), None, "head"),
        P(None, ("groups", "seq")),
        P("groups"),
    )
    out_specs = (
        P(("groups", "seq"), "head"),
        P("head", ("groups", "seq"), None),
        P("head", ("groups", "seq"), None),
    )
    return jax.shard_map(shards, mesh=mesh, in_specs=in_specs, out_specs=out_specs, check_vma=False)
```

```python
import functools
import heapq
import math

import jax
import jax.numpy as jnp
from jax import lax
from jax.experimental import pallas as pl
from jax.experimental.pallas import tpu as pltpu
from jax.sharding import PartitionSpec as P

HEAD_SIZE = 128
PRIOR_SEGMENTS = 2
PAGE_TOKENS = 16
QBLK = 64
KINDS = PRIOR_SEGMENTS + 1
CURRENT = PRIOR_SEGMENTS

rope_base = 1000000.0
masked_value = -1e30
MESH = pl.DeviceIdType.MESH
RIGHT, LEFT, ACROSS = 0, 1, 2
ONES_ROWS = 16
GRANT = 60 * 1024 * 1024

OWN0, OWN1, GUEST, SPARE = 0, 1, 2, 3
NOTHING, BATCH2, BATCH1, TURN, DIAGONAL, GUEST_TURN, PACK, RETURN, PAGES, MERGE = range(10)
FIELD = 128

WIRE, HOP, RELAY = 2.81, 1.9, 1.0
COST = {BATCH2: 2.6, BATCH1: 1.5, TURN: 4.0, DIAGONAL: 1.6, GUEST_TURN: 2.0, PACK: 0.8, PAGES: 1.3}


def offloaded(n, d):
    if d < n - 2 or n < 4:
        return set()
    return {
        (j, part, 0)
        for j in range(n - 2)
        for part in (0, CURRENT)
        if part < CURRENT or j <= n - 4
    }


def needed(n, groups, d):
    left = offloaded(n, d)
    return {
        (j, part, g)
        for j in range(n)
        for part in range(KINDS)
        for g in range(groups)
        if j != d and (part < CURRENT or j < d) and (j, part, g) not in left
    }


def route(n, groups):
    need = {d: needed(n, groups, d) for d in range(n)}
    here = {
        d: {(d, part, g): 0.0 for part in range(KINDS) for g in range(groups)} for d in range(n)
    }
    taken = {d: set(here[d]) for d in range(n)}
    lack = {}
    for d in range(n):
        for x in sorted(need[d]):
            lack[x] = lack.get(x, 0) + 1
    target = {}
    for d in range(n):
        if d + 2 < n:
            target[(d, RIGHT)] = d + 2
        if d - 2 >= 0:
            target[(d, LEFT)] = d - 2
        target[(d, ACROSS)] = d ^ 1
    wanted = {d - 2: offloaded(n, d) for d in range(n) if offloaded(n, d)}
    urgent = set().union(*wanted.values()) if wanted else set()
    free = {link: 0.0 for link in target}
    for h in wanted:
        free[(h + 2, LEFT)] = 3.5 * WIRE
    ready = {}
    returned = {}
    sends = {link: [] for link in target}
    arrivals = {d: {} for d in range(n)}
    events = []
    for k, link in enumerate(target):
        heapq.heappush(events, (free[link], k, 0, link))
    count = len(events)
    idle = set()

    def pick(link, now):
        u, v = link[0], target[link]
        if link[1] == RIGHT and u in wanted and u not in returned and ready.get(u, now + 1) <= now:
            return RETURN
        best = None
        for x in sorted(here[u]):
            if here[u][x] > now + 1e-9 or x in taken[v] or x not in need[v]:
                continue
            others = sum(1 for w in (v + 2, v - 2, v ^ 1) if 0 <= w < n and w != u and x in taken[w])
            score = lack[x] - SHARED * others
            if x in urgent and (v in wanted or (link[1] != LEFT and v < n - 4)):
                score += BONUS
            score += ((x[0] * 7 + x[1] * 5 + x[2] * 3 + u * 11 + link[1] * 13 + SALT) * 7919 % 101) / 101
            if best is None or score > best[0]:
                best = (score, x)
        return None if best is None else best[1]

    while events:
        now, _, kind, what = heapq.heappop(events)
        if kind == 0:
            link = what
            if free[link] > now + 1e-9:
                heapq.heappush(events, (free[link], count, 0, link))
                count += 1
                continue
            x = pick(link, now)
            if x is None:
                idle.add(link)
                continue
            v = target[link]
            if x == RETURN:
                returned[link[0]] = now + 3.6 * WIRE + HOP
                free[link] = now + 3.6 * WIRE
            else:
                taken[v].add(x)
                lack[x] -= 1
                sends[link].append(x)
                arrivals[v][x] = now + WIRE + HOP
                here[v][x] = now + WIRE + HOP + RELAY
                free[link] = now + WIRE
                heapq.heappush(events, (here[v][x], count, 1, v))
                count += 1
                if v in wanted and v not in ready and wanted[v] <= set(here[v]):
                    ready[v] = max(here[v][y] for y in wanted[v]) + 4.0
                    heapq.heappush(events, (ready[v], count, 1, v))
                    count += 1
            heapq.heappush(events, (free[link], count, 0, link))
            count += 1
        else:
            for link in sorted(x for x in idle if x[0] == what):
                idle.discard(link)
                heapq.heappush(events, (max(now, free[link]), count, 0, link))
                count += 1
    return sends, arrivals, wanted, returned


SALT, BONUS, SHARED = 16, 3.0, 2.0


def schedule(n, groups):
    sends, arrivals, wanted, returned = route(n, groups)
    tables = []
    for d in range(n):
        rows = []
        have = {(d, part, g) for part in range(KINDS) for g in range(groups)}
        queue = {way: list(sends.get((d, way), [])) for way in (RIGHT, LEFT, ACROSS)}
        order = sorted(arrivals[d], key=lambda x: (arrivals[d][x], x))
        guest = sorted(wanted.get(d, ()))
        pending = {OWN0: [], OWN1: [], GUEST: []}
        absorbed_guest = 0
        turned_guest = packed = sent_back = paged = False
        pages_left = {(j, 1, g) for j in range(n) for g in range(groups)} - have

        def ready_sends():
            out = {}
            for way, q in queue.items():
                if q and q[0] in have:
                    out[way] = q.pop(0)
            return out

        def emit(wait=None, op=NOTHING, pieces=(), accs=()):
            if wait is not None:
                have.add(wait)
            if wait is None and op != NOTHING and rows and rows[-1][2] == NOTHING:
                rows[-1][2:] = [op, list(pieces), list(accs)]
                return
            rows.append([wait, ready_sends(), op, list(pieces), list(accs)])
            while True:
                more = ready_sends()
                if not more:
                    break
                rows.append([None, more, NOTHING, [], []])

        def note(x):
            pages_left.discard(x)
            pending[x[2]].append(x)
            if x in guest:
                pending[GUEST].append(x)

        def streams(count, size):
            chosen = []
            for acc in (GUEST, OWN0, OWN1):
                if acc == GUEST and not turned_guest:
                    continue
                while len(pending[acc]) >= size and len(chosen) < count:
                    chosen.append((acc, [pending[acc].pop(0) for _ in range(size)]))
            return chosen

        def put_back(chosen):
            for acc, pieces in reversed(chosen):
                pending[acc] = pieces + pending[acc]

        def batch(op, chosen):
            nonlocal now, absorbed_guest
            pieces, accs = [], []
            for acc, some in chosen:
                pieces += some
                accs.append(acc)
                absorbed_guest += len(some) if acc == GUEST else 0
            emit(None, op, pieces, accs)
            now += COST[op]

        emit()
        emit(None, TURN)
        now = COST[TURN]
        for g in range(groups):
            for part in range(PRIOR_SEGMENTS):
                note((d, part, g))
            if (d, CURRENT, g) in guest:
                pending[GUEST].append((d, CURRENT, g))
        first = [(OWN0, [pending[OWN0].pop(0) for _ in range(2)]),
                 (OWN1, [pending[OWN1].pop(0) for _ in range(2)])]
        batch(BATCH2, first)
        emit(None, DIAGONAL)
        now += COST[DIAGONAL]
        guest_at = 3.5 * WIRE + HOP + 1.0
        while True:
            while order and arrivals[d][order[0]] <= now + 0.2:
                x = order.pop(0)
                emit(x)
                note(x)
            if guest and not turned_guest and guest_at <= now:
                emit(None, GUEST_TURN)
                now += COST[GUEST_TURN]
                turned_guest = True
                continue
            if packed and not sent_back:
                emit(None, RETURN)
                sent_back = True
                continue
            if guest and not packed and absorbed_guest == len(guest):
                emit(None, PACK)
                now += COST[PACK]
                packed = True
                continue
            chosen = streams(2, 2)
            if len(chosen) == 2:
                batch(BATCH2, chosen)
                continue
            put_back(chosen)
            last_guest = (
                guest and turned_guest and absorbed_guest + len(pending[GUEST]) == len(guest)
            )
            upcoming = arrivals[d][order[0]] if order else None
            if last_guest and pending[GUEST]:
                chosen = streams(2, 1)
                if len(chosen) == 1:
                    chosen.append((SPARE, list(chosen[0][1])))
                batch(BATCH1, chosen)
                continue
            if not pages_left and not paged:
                emit(None, PAGES)
                now += COST[PAGES]
                paged = True
                continue
            if guest and not turned_guest and (upcoming is None or guest_at <= upcoming):
                now = max(now, guest_at)
                continue
            if upcoming is None or upcoming - now > 1.2:
                chosen = streams(2, 1)
                if len(chosen) == 2:
                    batch(BATCH1, chosen)
                    continue
                if chosen and upcoming is None:
                    chosen.append((SPARE, list(chosen[0][1])))
                    batch(BATCH1, chosen)
                    continue
                put_back(chosen)
            if upcoming is None:
                break
            now = max(now, upcoming)
        if offloaded(n, d):
            emit(None, MERGE)
        assert not any(queue.values()) and not any(pending.values()) and paged
        tables.append(rows)
    length = max(len(rows) for rows in tables)

    def number(x):
        return (x[0] * KINDS + x[1]) * groups + x[2]

    packed_tables = []
    for rows in tables:
        words = []
        for wait, sent, op, pieces, accs in rows:
            first = [0 if wait is None else number(wait) + 1]
            first += [number(sent[way]) + 1 if way in sent else 0 for way in (RIGHT, LEFT, ACROSS)]
            listed = sum(number(x) * FIELD**k for k, x in enumerate(pieces))
            accs = list(accs) + [0] * (2 - len(accs))
            words.append((first + [op] + accs, listed))
        words += [([0] * 7, 0)] * (length - len(words))
        packed_tables.append(words)
    return length, packed_tables


def kernel(n, groups, per_group, length, tables, table_ref, remap_ref, q_hbm, *refs):
    stored, current = refs[:2], refs[2:4]
    (
        out_ref, paged_keys_ref, paged_values_ref,
        rows_ref, q_ref, mixed, turns, guest_q, guest_turns, cos_ref, sin_ref, held, turned, top, total,
        raw, back, back_stats, came, came_stats, own_sem, send_sem, recv_sem, side_send, side_recv,
    ) = refs[4:]
    me = lax.axis_index("seq")
    partner = me + 1 - 2 * (me % 2)
    tokens = q_hbm.shape[0]
    heads = groups * per_group
    blocks = tokens // QBLK
    scale = HEAD_SIZE ** -0.5 * math.log2(math.e)
    has_right = me + 2 < n
    has_left = me - 2 >= 0
    is_top = me >= n - 2
    is_helper = (me >= n - 4) & (me < n - 2)
    width = per_group * HEAD_SIZE

    def at(j, part, g):
        return (j * KINDS + part) * groups + g

    own = [pltpu.make_async_copy(q_hbm, q_ref, own_sem.at[0])]
    for kv in range(2):
        own.append(pltpu.make_async_copy(stored[kv], mixed.at[kv], own_sem.at[len(own)]))
    for g in range(groups):
        for kv in range(2):
            own.append(
                pltpu.make_async_copy(
                    current[kv].at[:, pl.ds(g * HEAD_SIZE, HEAD_SIZE)],
                    held.at[at(me, CURRENT, g), kv],
                    own_sem.at[len(own)],
                )
            )
    for copy in own:
        copy.start()
    barrier = pltpu.get_barrier_semaphore()
    pl.semaphore_signal(barrier, inc=1, device_id={"seq": partner}, device_id_type=MESH)

    @pl.when(has_right)
    def _():
        pl.semaphore_signal(barrier, inc=1, device_id={"seq": me + 2}, device_id_type=MESH)

    @pl.when(has_left)
    def _():
        pl.semaphore_signal(barrier, inc=1, device_id={"seq": me - 2}, device_id_type=MESH)

    lane = lax.broadcasted_iota(jnp.int32, (1, HEAD_SIZE), 1)
    power = (lane % (HEAD_SIZE // 2)).astype(jnp.float32) * (-2.0 * math.log2(rope_base) / HEAD_SIZE)
    frequency = jnp.exp2(power)
    for part in range(KINDS):
        for b in range(blocks):
            base = remap_ref[KINDS - 1 - part, b].astype(jnp.float32)
            turns[part * blocks + b : part * blocks + b + 1] = base * frequency
    if turns.shape[0] > KINDS * blocks:
        rest = turns.shape[0] - KINDS * blocks
        turns[KINDS * blocks :] = jnp.zeros((rest, HEAD_SIZE), jnp.float32)

    for d in range(n):

        @pl.when(me == d)
        def _():
            for k, (words, _) in enumerate(tables[d]):
                for c, word in enumerate(words):
                    rows_ref[c, k] = word * per_group if c > 4 else word

    for kv in range(2):
        own[1 + kv].wait()
        for part in range(PRIOR_SEGMENTS):
            for g in range(groups):
                held[at(me, part, g), kv] = mixed[
                    kv, :, part, g * HEAD_SIZE : (g + 1) * HEAD_SIZE
                ]

    top[...] = jnp.full(top.shape, masked_value, jnp.float32)

    def clear(h, carry):
        total[h] = jnp.zeros(total.shape[1:], jnp.float32)
        return carry

    lax.fori_loop(0, total.shape[0], clear, 0)

    expected = 1 + has_right.astype(jnp.int32) + has_left.astype(jnp.int32)
    pl.semaphore_wait(barrier, expected)

    def side(index, source, destination, target):
        return pltpu.make_async_remote_copy(
            src_ref=source,
            dst_ref=destination,
            send_sem=side_send.at[index],
            recv_sem=side_recv.at[index],
            device_id={"seq": target},
            device_id_type=MESH,
        )

    down = jnp.maximum(me - 2, 0)
    up = jnp.minimum(me + 2, n - 1)
    send_q = side(0, q_ref.at[:, pl.ds(0, width)], guest_q, down)
    send_turns = side(1, turns, guest_turns, down)
    send_back = side(2, back, came, up)
    send_stats = side(3, back_stats, came_stats, up)

    own[0].wait()

    @pl.when(is_top)
    def _():
        send_turns.start()
        send_q.start()

    for copy in own[3:]:
        copy.wait()

    def remote(way, piece):
        target = (me + 2, me - 2, partner)[way]
        return pltpu.make_async_remote_copy(
            src_ref=held.at[piece],
            dst_ref=held.at[piece],
            send_sem=send_sem.at[way, piece],
            recv_sem=recv_sem.at[piece],
            device_id={"seq": target},
            device_id_type=MESH,
        )

    def tables_of(ref):
        rows = lax.broadcasted_iota(jnp.int32, (QBLK, HEAD_SIZE), 0).astype(jnp.float32)
        angle = rows * frequency
        near_cos, near_sin = jnp.cos(angle), jnp.sin(angle)
        far = ref[...]
        far_cos, far_sin = jnp.cos(far), jnp.sin(far)
        lane = lax.broadcasted_iota(jnp.int32, (QBLK, HEAD_SIZE), 1)
        for part in range(KINDS):
            for b in range(blocks):
                r = part * blocks + b
                c, s = far_cos[r : r + 1], far_sin[r : r + 1]
                span = slice(b * QBLK, (b + 1) * QBLK)
                cos_ref[part, span] = c * near_cos - s * near_sin
                sin = s * near_cos + c * near_sin
                sin_ref[part, span] = jnp.where(lane < HEAD_SIZE // 2, -sin, sin)

    def turn(source, count, base):
        def one(part, carry):
            cos = cos_ref[part]
            sin = sin_ref[part]
            for h in range(count):
                x = source[:, h * HEAD_SIZE : (h + 1) * HEAD_SIZE].astype(jnp.float32)
                y = x * cos + pltpu.roll(x, HEAD_SIZE // 2, 1) * sin
                y = y.astype(jnp.bfloat16).astype(jnp.float32) * scale
                high = y.astype(jnp.bfloat16)
                low = (y - high.astype(jnp.float32)).astype(jnp.bfloat16)
                turned[part, base + h, :HEAD_SIZE] = high.T
                turned[part, base + h, HEAD_SIZE:] = low.T
            return carry

        lax.fori_loop(0, KINDS, one, 0)

    def absorb(streams, causal=False):
        ready = []
        for pieces, base, query in streams:
            keys = []
            for piece in pieces:
                k = held[piece, 0]
                keys.append((jnp.concatenate([k, k], 1), piece // groups % KINDS))
            values = jnp.concatenate([held[piece, 1] for piece in pieces], 0).T
            ones = jnp.ones((ONES_ROWS, values.shape[1]), jnp.bfloat16)
            ready.append((keys, jnp.concatenate([values, ones], 0), base, query))
        units = [(stream, h) for stream in ready for h in range(per_group)]

        def score(unit):
            (keys, _, _, query), h = unit
            some = [
                jnp.dot(k, turned[part, query + h], preferred_element_type=jnp.float32)
                for k, part in keys
            ]
            return some[0] if len(some) == 1 else jnp.concatenate(some, 0)

        def add(unit, weights, factor):
            (_, values, base, _), h = unit
            total[base + h] = total[base + h] * factor + jnp.dot(
                values, weights, preferred_element_type=jnp.float32
            )

        pending = []
        following = score(units[0])
        for k, unit in enumerate(units):
            scores = following
            if k + 1 < len(units):
                following = score(units[k + 1])
            if causal:
                key_index = lax.broadcasted_iota(jnp.int32, scores.shape, 0)
                row_index = lax.broadcasted_iota(jnp.int32, scores.shape, 1)
                scores = jnp.where(key_index <= row_index, scores, masked_value)
            (_, _, base, _), h = unit
            old = top[base + h]
            new = jnp.maximum(old, jnp.max(scores, 0, keepdims=True))
            factor = jnp.exp2(old - new)
            weights = jnp.exp2(scores - new).astype(jnp.bfloat16)
            top[base + h] = new
            if len(pending) == 2:
                add(*pending.pop(0))
            pending.append((unit, weights, factor))
        for some in pending:
            add(*some)

    rounds = tokens // PAGE_TOKENS // n
    here = n * rounds
    last = PRIOR_SEGMENTS - 1

    def pages():
        def collect(j, carry):
            for r in range(rounds):
                rows = pl.ds(pl.multiple_of((r * n + me) * PAGE_TOKENS, PAGE_TOKENS), PAGE_TOKENS)
                to = pl.ds(pl.multiple_of((j * rounds + r) * PAGE_TOKENS, PAGE_TOKENS), PAGE_TOKENS)
                for kv in range(2):
                    for g in range(groups):
                        raw[kv, to, g * HEAD_SIZE : (g + 1) * HEAD_SIZE] = held[
                            at(j, last, g), kv, rows, :
                        ]
            return carry

        lax.fori_loop(0, n, collect, 0)
        size = here * PAGE_TOKENS
        row = lax.broadcasted_iota(jnp.int32, (size, size), 0)
        column = lax.broadcasted_iota(jnp.int32, (size, size), 1)
        slot = lax.broadcasted_iota(jnp.int32, (1, size), 1) // PAGE_TOKENS
        page = jnp.zeros((1, size), jnp.int32)
        for k in range(here):
            j, r = k // rounds, k % rounds
            entry = table_ref[j * (tokens // PAGE_TOKENS) + r * n + me]
            page = jnp.where(slot == k, entry, page)
        chosen = (row % here == page) & (row // here == column % PAGE_TOKENS)
        pick = jnp.where(chosen, 1.0, 0.0).astype(jnp.bfloat16)
        for kv in range(2):
            moved = jnp.dot(pick, raw[kv], preferred_element_type=jnp.float32)
            moved = moved.astype(jnp.bfloat16)
            for g in range(groups):
                for t in range(PAGE_TOKENS):
                    (paged_keys_ref, paged_values_ref)[kv][g, :, t * HEAD_SIZE : (t + 1) * HEAD_SIZE] = moved[
                        t * here : (t + 1) * here, g * HEAD_SIZE : (g + 1) * HEAD_SIZE
                    ]

    guest_base = heads
    spare_base = heads + per_group

    listed = []
    for r in range(length):
        choice = None
        for d in range(n):
            value = tables[d][r][1]
            if value:
                choice = value if choice is None else jnp.where(me == d, value, choice)
        if choice is not None:
            listed.append((r, choice))

    def step(row, carry):
        wait, right, left, across, op, first, second = [rows_ref[c, row] for c in range(7)]

        @pl.when(wait > 0)
        def _():
            remote(RIGHT, wait - 1).wait_recv()

        @pl.when(right + left + across > 0)
        def _():
            for way, sent in ((ACROSS, across), (RIGHT, right), (LEFT, left)):

                @pl.when(sent > 0)
                def _():
                    remote(way, sent - 1).start()

        def streams(size):
            word = jnp.int32(0)
            for r, choice in listed:
                word = jnp.where(row == r, choice, word)
            some = []
            for k, base in enumerate((first, second)):
                pieces = [word // FIELD ** (k * size + i) % FIELD for i in range(size)]
                some.append((pieces, base, jnp.where(base == spare_base, 0, base)))
            return some

        @pl.when(op == BATCH2)
        def _():
            absorb(streams(2))

        @pl.when(op == BATCH1)
        def _():
            absorb(streams(1))

        @pl.when(op > BATCH1)
        def _():
            others(op)

        return carry

    def others(op):
        @pl.when(op == TURN)
        def _():
            tables_of(turns)
            turn(q_ref, heads, 0)

        @pl.when(op == DIAGONAL)
        def _():
            absorb(
                [([at(me, CURRENT, g)], g * per_group, g * per_group) for g in range(groups)], True
            )

        @pl.when(op == GUEST_TURN)
        def _():
            send_turns.wait_recv()
            send_q.wait_recv()
            tables_of(guest_turns)
            turn(guest_q, per_group, guest_base)

        @pl.when(op == PACK)
        def _():
            for h in range(per_group):
                part = total[guest_base + h]
                share = part[HEAD_SIZE : HEAD_SIZE + 1]
                back[h] = (part[:HEAD_SIZE] / share).astype(jnp.bfloat16)
                back_stats[0, h : h + 1] = top[guest_base + h]
                back_stats[1, h : h + 1] = share

        @pl.when(op == RETURN)
        def _():
            send_stats.start()
            send_back.start()

        @pl.when(op == PAGES)
        def _():
            pages()

        @pl.when(op == MERGE)
        def _():
            send_stats.wait_recv()
            send_back.wait_recv()
            for h in range(per_group):
                mine, other = top[h], came_stats[0, h : h + 1]
                new = jnp.maximum(mine, other)
                keep = jnp.exp2(mine - new)
                share = came_stats[1, h : h + 1] * jnp.exp2(other - new)
                total[h, :HEAD_SIZE] = (
                    total[h, :HEAD_SIZE] * keep + came[h].astype(jnp.float32) * share
                )
                total[h, HEAD_SIZE : HEAD_SIZE + 1] = (
                    total[h, HEAD_SIZE : HEAD_SIZE + 1] * keep + share
                )

    lax.fori_loop(0, length, step, 0)

    for h in range(heads):
        finished = total[h, :HEAD_SIZE] / total[h, HEAD_SIZE : HEAD_SIZE + 1]
        out_ref[:, h * HEAD_SIZE : (h + 1) * HEAD_SIZE] = finished.T.astype(out_ref.dtype)

    for d in range(n):

        @pl.when(me == d)
        def _():
            for words, _ in tables[d]:
                for way in (RIGHT, LEFT, ACROSS):
                    if words[1 + way]:
                        remote(way, words[1 + way] - 1).wait_send()

    @pl.when(is_top)
    def _():
        send_turns.wait_send()
        send_q.wait_send()

    @pl.when(is_helper)
    def _():
        send_stats.wait_send()
        send_back.wait_send()


def finish(*refs):
    half = len(refs) // 3
    copies = [
        pltpu.make_async_copy(refs[k], refs[half + k], refs[2 * half + k]) for k in range(half)
    ]
    for copy in copies:
        copy.start()
    for copy in copies:
        copy.wait()


def shards(
    queries, current_keys, current_values, stored_keys, stored_values, remap_table, block_table
):
    tokens, width = queries.shape
    key_width = current_keys.shape[1]
    groups = key_width // HEAD_SIZE
    heads = width // HEAD_SIZE
    per_group = heads // groups
    owners = lax.axis_size("seq")
    length, tables = schedule(owners, groups)
    pieces = owners * KINDS * groups
    blocks = tokens // QBLK
    rounds = tokens // PAGE_TOKENS // owners
    here = owners * rounds
    hbm = pl.BlockSpec(memory_space=pltpu.HBM)
    vmem = pl.BlockSpec(memory_space=pltpu.VMEM)
    smem = pl.BlockSpec(memory_space=pltpu.SMEM)
    slots = heads + 2 * per_group
    turn_rows = -(-KINDS * blocks // 8) * 8
    bf16, f32 = jnp.bfloat16, jnp.float32
    results = pl.pallas_call(
        functools.partial(kernel, owners, groups, per_group, length, tables),
        out_shape=(
            pltpu.VMEM((tokens, width), bf16),
            pltpu.VMEM((groups, here, PAGE_TOKENS * HEAD_SIZE), bf16),
            pltpu.VMEM((groups, here, PAGE_TOKENS * HEAD_SIZE), bf16),
        ),
        in_specs=[smem, smem] + [hbm] * 5,
        out_specs=(vmem, vmem, vmem),
        scratch_shapes=[
            pltpu.SMEM((7, length), jnp.int32),
            pltpu.VMEM((tokens, width), bf16),
            pltpu.VMEM((2, tokens, PRIOR_SEGMENTS, key_width), bf16),
            pltpu.VMEM((turn_rows, HEAD_SIZE), f32),
            pltpu.VMEM((tokens, per_group * HEAD_SIZE), bf16),
            pltpu.VMEM((turn_rows, HEAD_SIZE), f32),
            pltpu.VMEM((KINDS, tokens, HEAD_SIZE), f32),
            pltpu.VMEM((KINDS, tokens, HEAD_SIZE), f32),
            pltpu.VMEM((pieces, 2, tokens, HEAD_SIZE), bf16),
            pltpu.VMEM((KINDS, heads + per_group, 2 * HEAD_SIZE, tokens), bf16),
            pltpu.VMEM((slots, 1, tokens), f32),
            pltpu.VMEM((slots, HEAD_SIZE + ONES_ROWS, tokens), f32),
            pltpu.VMEM((2, here * PAGE_TOKENS, key_width), bf16),
            pltpu.VMEM((per_group, HEAD_SIZE, tokens), bf16),
            pltpu.VMEM((2, per_group, tokens), f32),
            pltpu.VMEM((per_group, HEAD_SIZE, tokens), bf16),
            pltpu.VMEM((2, per_group, tokens), f32),
            pltpu.SemaphoreType.DMA((3 + 2 * groups,)),
            pltpu.SemaphoreType.DMA((3, pieces)),
            pltpu.SemaphoreType.DMA((pieces,)),
            pltpu.SemaphoreType.DMA((4,)),
            pltpu.SemaphoreType.DMA((4,)),
        ],
        compiler_params=pltpu.CompilerParams(
            collective_id=0, has_side_effects=True, vmem_limit_bytes=GRANT
        ),
    )(block_table, remap_table, queries, stored_keys, stored_values, current_keys, current_values)
    return pl.pallas_call(
        finish,
        out_shape=tuple(jax.ShapeDtypeStruct(x.shape, x.dtype) for x in results),
        in_specs=[vmem] * 3,
        out_specs=(hbm,) * 3,
        scratch_shapes=[pltpu.SemaphoreType.DMA] * 3,
        compiler_params=pltpu.CompilerParams(vmem_limit_bytes=8 * 1024 * 1024),
    )(*results)


def solution(mesh):
    in_specs = (
        P(("groups", "seq"), "head"),
        P(("groups", "seq"), "head"),
        P(("groups", "seq"), "head"),
        P(("groups", "seq"), None, "head"),
        P(("groups", "seq"), None, "head"),
        P(None, ("groups", "seq")),
        P("groups"),
    )
    out_specs = (
        P(("groups", "seq"), "head"),
        P("head", ("groups", "seq"), None),
        P("head", ("groups", "seq"), None),
    )
    return jax.shard_map(shards, mesh=mesh, in_specs=in_specs, out_specs=out_specs, check_vma=False)
```
